32 devices in a mesh: hist: 4 (over z), rows: 2 (over y), dom: 4 (over x, core).
Axes of the slice: x: 2, y: 2, z: 4, core: 2. Of those that a mesh axis runs over, the one named last changes fastest.
Arguments:
- row_index: int32 [4, 32768], P(None, ('hist', 'rows', 'dom')), may hold values from 0 to 510
- col_index: int32 [4, 32768], P(None, ('hist', 'rows', 'dom')), may hold values from 0 to 510
- bin_index: int32 [4, 32768], P(None, ('hist', 'rows', 'dom')), may hold values from 0 to 255
- charge: bfloat16 [32768], P(('hist', 'rows', 'dom')), may hold values from 0.5 to 2
- momentum: float32 [2, 32768], P(None, ('hist', 'rows', 'dom')), may hold values from -6 to 6
- history: bfloat16 [32, 512, 512], P('hist', 'rows'), may hold values from 0 to 2
- kernel_cols: bfloat16 [32, 512, 512], P('hist', 'dom'), may hold values from -0.25 to 0.25
- kernel_rows: bfloat16 [32, 512, 2, 512], P('hist', 'rows'), may hold values from -0.046875 to 0.046875
Outputs:
- momentum_out: float32 [2, 32768], P(None, ('hist', 'rows', 'dom'))
- history_out: bfloat16 [32, 512, 512], P('hist', 'rows')
The draws below stay inside these ranges and needn't reach their ends.
All inputs are finite; a program needn't handle non-finite values.
Results may differ from the reference program's by a relative error of at most 0.0024.
Values may be sent and summed in bfloat16 or wider, within the bound.
A program may use at most 64 MiB of HBM per device.

```python
import math
import jax
import jax.numpy as jnp
from jax import lax

NG = 512
BINS = 16
STEPS = 4
LAGS = 32
PARTICLES = 32768


def draw_row_index(key, part):
    shuffled = jax.random.permutation(jax.random.fold_in(key, 7), PARTICLES).astype(jnp.int32)
    centre = shuffled * (NG - 1) // PARTICLES
    drift_rows = jnp.arange(STEPS, dtype=jnp.int32)[:, None] - STEPS // 2
    jitter = jax.random.randint(jax.random.fold_in(key, 11), (STEPS, PARTICLES), -4, 5, dtype=jnp.int32)
    return jnp.clip(centre[None, :] + drift_rows + jitter, 0, NG - 2).astype(jnp.int32)


def set_ends(result, rng, smallest, high):
    extent = result.shape
    index_at = [jax.random.randint(jax.random.fold_in(rng, axis), (), 0, extent[axis]) for axis in range(len(extent))]
    result = result.at[tuple(index_at)].set(smallest)
    longest = extent.index(max(extent))
    index_at[longest] = (index_at[longest] + 1) % extent[longest]
    return result.at[tuple(index_at)].set(high)


def levels(key, dims, pieces, low, high):
    loudness, own = 1.0, jax.random.fold_in(key, 6)
    for position, blocks in pieces:
        draws = jnp.exp(jax.random.uniform(jax.random.fold_in(own, position), (blocks,), jnp.float32, low / len(pieces), high / len(pieces)))
        loudness = loudness * jnp.repeat(draws, dims[position] // blocks).reshape([-1 if axis == position else 1 for axis in range(len(dims))])
    return loudness


def noise(key, extent, deviation, limit, pieces=(), kind=jnp.bfloat16):
    drawn = jax.random.normal(key, extent, jnp.float32) * deviation
    if len(pieces) > 0:
        drawn = levels(key, extent, pieces, -0.22, 0.18) * drawn
    return jnp.clip(drawn, min=-limit, max=limit).astype(kind)


def setup_inputs(seed: int = 0) -> dict:
    arg_keys = jax.random.split(jax.random.key(seed), 9)
    row_index = draw_row_index(jax.random.fold_in(arg_keys[8], 71), 0)
    col_index = set_ends(jax.random.randint(arg_keys[1], (STEPS, PARTICLES), 0, NG - 1), jax.random.fold_in(arg_keys[1], 1), 0, (NG - 1) - 1).astype(jnp.int32)
    bin_index = set_ends(jax.random.randint(arg_keys[2], (STEPS, PARTICLES), 0, BINS * BINS), jax.random.fold_in(arg_keys[2], 1), 0, (BINS * BINS) - 1).astype(jnp.int32)
    charge = jnp.clip(jnp.exp(math.log(2.0) - 1.3862944 * jax.random.uniform(arg_keys[3], (PARTICLES,), jnp.float32) ** levels(arg_keys[3], (PARTICLES,), ((0, 32),), -0.2, 0.2)), 0.5, 2.0).astype(jnp.bfloat16)
    momentum = noise(arg_keys[4], (2, PARTICLES), 1.0, 6.0, ((1, 32),), jnp.float32)
    history = jnp.clip(2.0 * jax.random.uniform(arg_keys[5], (LAGS, NG, NG), jnp.float32) ** levels(arg_keys[5], (LAGS, NG, NG), ((0, 4), (1, 2)), -0.2, 0.2), 0.0, 2.0).astype(jnp.bfloat16)
    kernel_cols = noise(arg_keys[6], (LAGS, NG, NG), NG ** -0.5, 0.25, ((0, 4), (1, 4)))
    kernel_rows = noise(arg_keys[7], (LAGS, NG, 2, NG), (NG * LAGS) ** -0.5, 0.046875, ((0, 4), (1, 2)))
    return {"row_index": row_index, "col_index": col_index, "bin_index": bin_index, "charge": charge, "momentum": momentum, "history": history, "kernel_cols": kernel_cols, "kernel_rows": kernel_rows}


kick_scale = 0.5


def rounded(values):
    return lax.optimization_barrier(values.astype(jnp.bfloat16)).astype(jnp.float32)


def reference(row_index, col_index, bin_index, charge, momentum, history, kernel_cols, kernel_rows):
    charge_f = charge.astype(jnp.float32)
    cols_wide = kernel_cols.astype(jnp.float32)
    rows_wide = kernel_rows.astype(jnp.float32)
    cycle_now = history
    kick_sum = jnp.zeros((PARTICLES, 2), jnp.float32)
    for turn_index in range(STEPS):
        row_now = row_index[turn_index].astype(jnp.int32)
        col_now = col_index[turn_index].astype(jnp.int32)
        bin_now = bin_index[turn_index]
        frac_row = ((bin_now // BINS).astype(jnp.float32) + 0.5) / BINS
        frac_col = ((bin_now % BINS).astype(jnp.float32) + 0.5) / BINS
        lower = rounded(charge_f * (1.0 - frac_row))
        upper = rounded(charge_f * frac_row)
        density = jnp.zeros((NG, NG), jnp.float32)
        density = density.at[row_now, col_now].add(lower * (1.0 - frac_col))
        density = density.at[row_now, col_now + 1].add(lower * frac_col)
        density = density.at[row_now + 1, col_now].add(upper * (1.0 - frac_col))
        density = density.at[row_now + 1, col_now + 1].add(upper * frac_col)
        newest = density.astype(jnp.bfloat16)
        cycle_now = jnp.concatenate([newest[None], cycle_now[:-1]], axis=0)
        mixed_rows = jnp.einsum("kab,kjb->kaj", cycle_now.astype(jnp.float32), cols_wide).astype(jnp.bfloat16)
        field_full = rounded(jnp.einsum("kaci,kaj->icj", rows_wide, mixed_rows.astype(jnp.float32)))
        corner_aa = field_full[row_now, :, col_now]
        corner_ba = field_full[row_now + 1, :, col_now]
        corner_ab = field_full[row_now, :, col_now + 1]
        corner_bb = field_full[row_now + 1, :, col_now + 1]
        weight_row = frac_row[:, None]
        weight_col = frac_col[:, None]
        near_col = (1.0 - weight_row) * corner_aa + weight_row * corner_ba
        far_col = (1.0 - weight_row) * corner_ab + weight_row * corner_bb
        kick_sum = kick_sum + ((1.0 - weight_col) * near_col + weight_col * far_col)
    momentum_out = momentum + kick_scale * kick_sum.T
    return momentum_out, cycle_now
```

```python
import functools
import jax
import jax.numpy as jnp
from jax import lax
from jax.experimental import pallas as pl
from jax.experimental.pallas import tpu as pltpu
from jax.sharding import PartitionSpec as P

NG = 512
BINS = 16
STEPS = 4
CORES = 2
PIECES = 8
kick_scale = 0.5

MESH = pl.DeviceIdType.MESH
VM = pl.BlockSpec(memory_space=pltpu.VMEM)
NT = (((1,), (1,)), ((), ()))


def place():
    return lax.axis_index("hist"), lax.axis_index("rows"), lax.axis_index("dom")


def hat(first, extent, where):
    places = lax.broadcasted_iota(jnp.int32, (extent, where.shape[1]), 0) + first
    gap = (places.astype(jnp.float32) - where).astype(jnp.bfloat16)
    return jnp.maximum(jnp.bfloat16(1.0) - jnp.abs(gap), jnp.bfloat16(0.0))


def plane_peer(rows, dom, shift):
    h, r, d = place()
    other = lax.rem(r * dom + d + shift, rows * dom)
    return other, (h, other // dom, lax.rem(other, dom))


def plane_barrier(rows, dom):
    barrier = pltpu.get_barrier_semaphore()
    for shift in range(1, rows * dom):
        pl.semaphore_signal(barrier, inc=1, device_id=plane_peer(rows, dom, shift)[1], device_id_type=MESH)
    pl.semaphore_wait(barrier, rows * dom - 1)


def gather_kernel(rows, dom, row_ref, col_ref, bin_ref, charge_ref, spots, out, charges, total,
                  send, recv, send_c, recv_c):
    _, r, d = place()
    n = rows * dom
    _, band, width = out.shape
    bins = bin_ref[...]
    row_bin = bins // BINS
    spots[0, 0:STEPS] = row_ref[...].astype(jnp.float32) + (row_bin.astype(jnp.float32) + 0.5) / BINS
    spots[0, STEPS:] = col_ref[...].astype(jnp.float32) + ((bins - row_bin * BINS).astype(jnp.float32) + 0.5) / BINS
    charges[0] = charge_ref[...]
    plane_barrier(rows, dom)

    def pair(shift):
        _, device = plane_peer(rows, dom, shift)
        return (
            pltpu.make_async_remote_copy(
                src_ref=spots.at[0], dst_ref=spots.at[shift], send_sem=send.at[shift], recv_sem=recv.at[shift],
                device_id=device, device_id_type=MESH),
            pltpu.make_async_remote_copy(
                src_ref=charge_ref, dst_ref=charges.at[shift], send_sem=send_c.at[shift],
                recv_sem=recv_c.at[shift], device_id=device, device_id_type=MESH))

    for shift in range(1, n):
        for copy in pair(shift):
            copy.start()
    total[...] = jnp.zeros_like(total)

    def add(shift):
        charge = charges[shift].astype(jnp.bfloat16)
        for s in range(STEPS):
            row = hat(r * band, band, spots[shift, s:s + 1, :]) * charge
            col = hat(d * width, width, spots[shift, STEPS + s:STEPS + s + 1, :])
            total[STEPS - 1 - s] += lax.dot_general(row, col, NT, preferred_element_type=jnp.float32)

    add(0)

    def step(shift, carry):
        for copy in pair(shift):
            copy.wait_recv()
        add(shift)
        return carry

    lax.fori_loop(1, n, step, 0)
    out[...] = total[...].astype(out.dtype)
    for shift in range(1, n):
        for copy in pair(shift):
            copy.wait_send()


def deposit(row_index, col_index, bin_index, charge, rows, dom, band, width):
    n = rows * dom
    own = row_index.shape[1]
    tile = (STEPS, band, width)
    return pl.pallas_call(
        functools.partial(gather_kernel, rows, dom),
        out_shape=(jax.ShapeDtypeStruct((n, 2 * STEPS, own), jnp.float32),
                   jax.ShapeDtypeStruct(tile, jnp.bfloat16)),
        in_specs=[VM] * 4, out_specs=(VM, VM),
        scratch_shapes=[pltpu.VMEM((n, 1, own), charge.dtype), pltpu.VMEM(tile, jnp.float32)]
        + [pltpu.SemaphoreType.DMA((n,))] * 4,
        compiler_params=pltpu.CompilerParams(collective_id=1, has_side_effects=True),
    )(row_index, col_index, bin_index, charge)


def shift_kernel(hist, rows, dom, part, tail, out, arrived, summed,
                 sem_hs, sem_hr, sem_cs, sem_cr, sem_xs, sem_xr, sem_ps, sem_pr, sem_fs, sem_fr):
    h, r, d = place()
    chips = dom // CORES
    up, down = (h + 1, r, d), (h - 1, r, d)
    partner = (h, r, d + 1 - 2 * lax.rem(d, CORES))
    is_first, is_last = h == 0, h == hist - 1
    barrier = pltpu.get_barrier_semaphore()

    @pl.when(jnp.logical_not(is_last))
    def _():
        pl.semaphore_signal(barrier, inc=1, device_id=up, device_id_type=MESH)

    @pl.when(jnp.logical_not(is_first))
    def _():
        pl.semaphore_signal(barrier, inc=1, device_id=down, device_id_type=MESH)

    across = [(h, r, lax.rem(d + CORES * j, dom)) for j in range(1, chips)]
    pl.semaphore_signal(barrier, inc=1, device_id=partner, device_id_type=MESH)
    for device in across:
        pl.semaphore_signal(barrier, inc=1, device_id=device, device_id_type=MESH)
    count = chips + jnp.where(is_first, 0, 1) + jnp.where(is_last, 0, 1)
    pl.semaphore_wait(barrier, count)

    def remote(src, dst, s_sem, r_sem, device):
        return pltpu.make_async_remote_copy(src_ref=src, dst_ref=dst, send_sem=s_sem, recv_sem=r_sem,
                                            device_id=device, device_id_type=MESH)

    def tail_copy(c):
        width = part.shape[2]
        columns = pl.ds(pl.multiple_of(d * width, width), width)
        return remote(tail.at[tail.shape[0] - STEPS + c, :, columns], out.at[d, c], sem_hs.at[c], sem_hr.at[c], up)

    def chain_copy(src, c):
        return remote(src.at[c], arrived.at[c], sem_cs.at[c], sem_cr.at[c], down)

    def cross_copy(c, j):
        return remote(out.at[d, c], out.at[d, c], sem_xs.at[c, j], sem_xr.at[c, j], across[j - 1])

    def partner_copy(c):
        return remote(out.at[d, c], out.at[d, c], sem_ps.at[c], sem_pr.at[c], partner)

    def forward_copy(c, j):
        other = lax.rem(d + CORES * (chips - j), dom)
        return remote(out.at[other, c], out.at[other, c], sem_fs.at[c, j], sem_fr.at[c, j], partner)

    @pl.when(is_last)
    def _():
        for c in range(STEPS):
            chain_copy(part, c).start()

    @pl.when(jnp.logical_not(is_last))
    def _():
        for c in range(STEPS):
            tail_copy(c).start()

    for c in range(STEPS):
        @pl.when(jnp.logical_not(is_last))
        def _():
            chain_copy(part, c).wait_recv()
            both = part[c].astype(jnp.float32) + arrived[c].astype(jnp.float32)

            @pl.when(is_first)
            def _():
                out[d, c] = both.astype(out.dtype)

            @pl.when(jnp.logical_not(is_first))
            def _():
                summed[c] = both.astype(out.dtype)
                chain_copy(summed, c).start()

        @pl.when(jnp.logical_not(is_first))
        def _():
            tail_copy(c).wait_recv()

        for j in range(1, chips):
            cross_copy(c, j).start()
        partner_copy(c).start()
    for c in range(STEPS):
        for j in range(1, chips):
            cross_copy(c, j).wait_recv()
            forward_copy(c, j).start()
    for c in range(STEPS):
        partner_copy(c).wait()
        for j in range(1, chips):
            forward_copy(c, j).wait()
            cross_copy(c, j).wait_send()

    @pl.when(jnp.logical_not(is_first))
    def _():
        for c in range(STEPS):
            chain_copy(part, c).wait_send()

    @pl.when(jnp.logical_not(is_last))
    def _():
        for c in range(STEPS):
            tail_copy(c).wait_send()


def newest_grids(part, tail, hist, rows, dom):
    chips = dom // CORES
    dma = pltpu.SemaphoreType.DMA
    return pl.pallas_call(
        functools.partial(shift_kernel, hist, rows, dom),
        out_shape=jax.ShapeDtypeStruct((dom,) + part.shape, part.dtype),
        in_specs=[VM, pl.BlockSpec(memory_space=pl.ANY)], out_specs=VM,
        scratch_shapes=[pltpu.VMEM(part.shape, part.dtype)] * 2
        + [dma((STEPS,))] * 4 + [dma((STEPS, chips))] * 2 + [dma((STEPS,))] * 2 + [dma((STEPS, chips))] * 2,
        compiler_params=pltpu.CompilerParams(collective_id=2, has_side_effects=True),
    )(part, tail)


def field_kernel(rows, new_ref, old_ref, cols_ref, rows_ref, out, own_out, cycle_out, grids, total):
    k = pl.program_id(0)
    lags = pl.num_programs(0)
    dom, _, band, width = new_ref.shape
    count = old_ref.shape[0]
    piece = NG // rows

    @pl.when(k == 0)
    def _():
        for d in range(dom):
            grids[0:STEPS, :, d * width:(d + 1) * width] = new_ref[d]
        grids[STEPS:] = old_ref[...]
        cycle_out[...] = grids[0:count]
        total[...] = jnp.zeros_like(total)

    window = grids[pl.ds(k, STEPS)].reshape(STEPS * band, NG)
    mixed = lax.dot_general(cols_ref[0], window, NT, preferred_element_type=jnp.float32).astype(jnp.bfloat16)
    stacked = jnp.concatenate(
        [mixed[:, (STEPS - 1 - s) * band:(STEPS - s) * band] for s in range(STEPS)], axis=0)
    for comp in range(2):
        total[comp] += jnp.dot(stacked, rows_ref[0, comp], preferred_element_type=jnp.float32)

    @pl.when(k == lags - 1)
    def _():
        for r in range(rows):
            block = jnp.concatenate([total[comp, :, r * piece:(r + 1) * piece] for comp in range(2)], axis=1)
            out[r] = block.astype(out.dtype)

            @pl.when(lax.axis_index("rows") == r)
            def _():
                own_out[...] = block


def field_parts(new, old, kernel_cols, rows_t, rows):
    lags, width, _ = kernel_cols.shape
    band = old.shape[1]
    return pl.pallas_call(
        functools.partial(field_kernel, rows),
        grid=(lags,),
        out_shape=(jax.ShapeDtypeStruct((rows, STEPS * width, 2 * NG // rows), jnp.bfloat16),
                   jax.ShapeDtypeStruct((STEPS * width, 2 * NG // rows), jnp.float32),
                   jax.ShapeDtypeStruct(old.shape, old.dtype)),
        in_specs=[pl.BlockSpec(new.shape, lambda k: (0, 0, 0, 0)),
                  pl.BlockSpec(old.shape, lambda k: (0, 0, 0)),
                  pl.BlockSpec((1, width, NG), lambda k: (k, 0, 0)),
                  pl.BlockSpec((1, 2, band, NG), lambda k: (k, 0, 0, 0))],
        out_specs=(pl.BlockSpec((rows, STEPS * width, 2 * NG // rows), lambda k: (0, 0, 0)),
                   pl.BlockSpec((STEPS * width, 2 * NG // rows), lambda k: (0, 0)),
                   pl.BlockSpec(old.shape, lambda k: (0, 0, 0))),
        scratch_shapes=[pltpu.VMEM((lags + STEPS, band, NG), old.dtype),
                        pltpu.VMEM((2, STEPS * width, NG), jnp.float32)],
    )(new, old, kernel_cols, rows_t)


def sum_kernel(hist, rows, dom, parts, own, spots, momentum, out, got, mine, from_low, from_high, to_high, to_low,
               kicks, got_kicks, sem_ys, sem_yr, sem_us, sem_ur, sem_ds, sem_dr, sem_ks, sem_kr):
    h, r, d = place()
    n = rows * dom
    tall, wide = own.shape
    width, band = tall // STEPS, wide // 2
    size = tall // PIECES
    kind = parts.dtype
    up, down = (h + 1, r, d), (h - 1, r, d)
    is_first, is_last = h == 0, h == hist - 1
    inner = jnp.logical_and(h > 0, h < hist - 1)
    barrier = pltpu.get_barrier_semaphore()

    @pl.when(jnp.logical_not(is_last))
    def _():
        pl.semaphore_signal(barrier, inc=1, device_id=up, device_id_type=MESH)

    @pl.when(jnp.logical_not(is_first))
    def _():
        pl.semaphore_signal(barrier, inc=1, device_id=down, device_id_type=MESH)

    for shift in range(1, n):
        pl.semaphore_signal(barrier, inc=1, device_id=plane_peer(rows, dom, shift)[1], device_id_type=MESH)
    pl.semaphore_wait(barrier, n - 1 + jnp.where(is_first, 0, 1) + jnp.where(is_last, 0, 1))

    def span(c):
        return pl.ds(pl.multiple_of(c * size, size), size)

    def row_copy(c, j):
        other = lax.rem(r + j, rows)
        return pltpu.make_async_remote_copy(
            src_ref=parts.at[other, span(c)], dst_ref=got.at[j, span(c)], send_sem=sem_ys.at[c, j],
            recv_sem=sem_yr.at[c, j], device_id=(h, other, d), device_id_type=MESH)

    def up_copy(c):
        return pltpu.make_async_remote_copy(
            src_ref=to_high.at[span(c)], dst_ref=from_low.at[span(c)], send_sem=sem_us.at[c],
            recv_sem=sem_ur.at[c], device_id=up, device_id_type=MESH)

    def down_copy(c):
        return pltpu.make_async_remote_copy(
            src_ref=to_low.at[span(c)], dst_ref=from_high.at[span(c)], send_sem=sem_ds.at[c],
            recv_sem=sem_dr.at[c], device_id=down, device_id_type=MESH)

    for c in range(PIECES):
        for j in range(1, rows):
            row_copy(c, j).start()

    kicks[...] = jnp.zeros_like(kicks)

    def kick(s):
        rows_s = pl.ds(pl.multiple_of(s * width, width), width)
        value = mine[rows_s]
        stacked = jnp.concatenate([value[:, :band], value[:, band:]], axis=0)
        coarse = stacked.astype(kind)
        fine = (stacked - coarse.astype(jnp.float32)).astype(kind)
        table = jnp.concatenate([coarse, fine], axis=0)

        def block(k, carry):
            row = hat(r * band, band, spots[k, pl.ds(s, 1), :])
            col = hat(d * width, width, spots[k, pl.ds(STEPS + s, 1), :]).astype(jnp.float32)
            along = jnp.dot(table, row, preferred_element_type=jnp.float32)
            for comp in range(2):
                both = (along[comp * width:(comp + 1) * width]
                        + along[(2 + comp) * width:(3 + comp) * width])
                kicks[k, comp:comp + 1, :] += jnp.sum(both * col, axis=0, keepdims=True)
            return carry

        lax.fori_loop(0, n, block, 0)

    lag = 2 * (hist - 2)
    group = PIECES // STEPS

    def step(t, carry):
        @pl.when(t < PIECES)
        def _():
            value = own[span(t)]
            for j in range(1, rows):
                row_copy(t, j).wait_recv()
                value += got[j, span(t)].astype(jnp.float32)
            mine[span(t)] = value

            @pl.when(is_first)
            def _():
                to_high[span(t)] = value.astype(kind)
                up_copy(t).start()

            @pl.when(is_last)
            def _():
                to_low[span(t)] = value.astype(kind)
                down_copy(t).start()

        low = t - 2 * h

        @pl.when(jnp.logical_and(inner, jnp.logical_and(low >= 0, low < PIECES)))
        def _():
            up_copy(low).wait_recv()
            to_high[span(low)] = (mine[span(low)] + from_low[span(low)].astype(jnp.float32)).astype(kind)
            up_copy(low).start()

        high = t - 2 * (hist - 1 - h)

        @pl.when(jnp.logical_and(inner, jnp.logical_and(high >= 0, high < PIECES)))
        def _():
            down_copy(high).wait_recv()
            to_low[span(high)] = (mine[span(high)] + from_high[span(high)].astype(jnp.float32)).astype(kind)
            down_copy(high).start()

        done = t - lag

        @pl.when(done >= 0)
        def _():
            @pl.when(is_first)
            def _():
                down_copy(done).wait_recv()
                mine[span(done)] = mine[span(done)] + from_high[span(done)].astype(jnp.float32)

            @pl.when(is_last)
            def _():
                up_copy(done).wait_recv()
                mine[span(done)] = mine[span(done)] + from_low[span(done)].astype(jnp.float32)

            @pl.when(inner)
            def _():
                mine[span(done)] = (mine[span(done)] + from_low[span(done)].astype(jnp.float32)
                                    + from_high[span(done)].astype(jnp.float32))

            @pl.when(lax.rem(done, group) == group - 1)
            def _():
                kick(done // group)

        return carry

    lax.fori_loop(0, PIECES + lag, step, 0)

    def kick_copy(k):
        _, device = plane_peer(rows, dom, n - k)
        return pltpu.make_async_remote_copy(
            src_ref=kicks.at[k], dst_ref=got_kicks.at[k], send_sem=sem_ks.at[k], recv_sem=sem_kr.at[k],
            device_id=device, device_id_type=MESH)

    for k in range(1, n):
        kick_copy(k).start()

    def finish(c, carry):
        @pl.when(jnp.logical_not(is_last))
        def _():
            up_copy(c).wait_send()

        @pl.when(jnp.logical_not(is_first))
        def _():
            down_copy(c).wait_send()

        for j in range(1, rows):
            row_copy(c, j).wait_send()
        return carry

    lax.fori_loop(0, PIECES, finish, 0)
    total = kicks[0]
    for k in range(1, n):
        kick_copy(k).wait()
        total = total + got_kicks[k]
    out[...] = momentum[...] + kick_scale * total


def sum_and_kick(parts, own, spots, momentum, hist, rows, dom):
    tall, wide = own.shape
    n = rows * dom
    dma = pltpu.SemaphoreType.DMA
    flat = pltpu.VMEM((tall, wide), parts.dtype)
    each = pltpu.VMEM((n,) + momentum.shape, momentum.dtype)
    return pl.pallas_call(
        functools.partial(sum_kernel, hist, rows, dom),
        out_shape=jax.ShapeDtypeStruct(momentum.shape, momentum.dtype),
        in_specs=[VM] * 4, out_specs=VM,
        scratch_shapes=[pltpu.VMEM(parts.shape, parts.dtype), pltpu.VMEM((tall, wide), jnp.float32),
                        flat, flat, flat, flat, each, each]
        + [dma((PIECES, rows))] * 2 + [dma((PIECES,))] * 4 + [dma((n,))] * 2,
        compiler_params=pltpu.CompilerParams(collective_id=3, has_side_effects=True),
    )(parts, own, spots, momentum)


def local(hist, rows, dom, row_index, col_index, bin_index, charge, momentum, history, kernel_cols, kernel_rows):
    band = history.shape[1]
    width = kernel_cols.shape[1]
    spots, part = deposit(row_index, col_index, bin_index, charge.astype(jnp.float32)[None], rows, dom, band, width)
    new = newest_grids(part, history, hist, rows, dom)
    rows_t = jnp.transpose(kernel_rows, (0, 2, 1, 3))
    parts, own, cycle_now = field_parts(new, history, kernel_cols, rows_t, rows)
    return sum_and_kick(parts, own, spots, momentum, hist, rows, dom), cycle_now


def solution(mesh):
    spread = ("hist", "rows", "dom")
    in_specs = (P(None, spread), P(None, spread), P(None, spread), P(spread), P(None, spread),
                P("hist", "rows", None), P("hist", "dom", None), P("hist", "rows", None, None))
    out_specs = (P(None, spread), P("hist", "rows", None))
    sizes = mesh.shape
    body = functools.partial(local, sizes["hist"], sizes["rows"], sizes["dom"])
    return jax.shard_map(body, mesh=mesh, in_specs=in_specs, out_specs=out_specs, check_vma=False)
```

```python
import functools
import jax
import jax.numpy as jnp
from jax import lax
from jax.experimental import pallas as pl
from jax.experimental.pallas import tpu as pltpu
from jax.sharding import PartitionSpec as P

NG = 512
BINS = 16
STEPS = 4
CORES = 2
PIECES = 8
kick_scale = 0.5

MESH = pl.DeviceIdType.MESH
VM = pl.BlockSpec(memory_space=pltpu.VMEM)
NT = (((1,), (1,)), ((), ()))


def place():
    return lax.axis_index("hist"), lax.axis_index("rows"), lax.axis_index("dom")


def hat(first, extent, where):
    places = lax.broadcasted_iota(jnp.int32, (extent, where.shape[1]), 0) + first
    gap = (places.astype(jnp.float32) - where).astype(jnp.bfloat16)
    return jnp.maximum(jnp.bfloat16(1.0) - jnp.abs(gap), jnp.bfloat16(0.0))


def plane_peer(rows, dom, shift):
    h, r, d = place()
    other = lax.rem(r * dom + d + shift, rows * dom)
    return other, (h, other // dom, lax.rem(other, dom))


def plane_barrier(rows, dom):
    barrier = pltpu.get_barrier_semaphore()
    for shift in range(1, rows * dom):
        pl.semaphore_signal(barrier, inc=1, device_id=plane_peer(rows, dom, shift)[1], device_id_type=MESH)
    pl.semaphore_wait(barrier, rows * dom - 1)


def gather_kernel(rows, dom, row_ref, col_ref, bin_ref, charge_ref, spots, out, charges, total,
                  send, recv, send_c, recv_c):
    _, r, d = place()
    n = rows * dom
    _, band, width = out.shape
    bins = bin_ref[...]
    row_bin = bins // BINS
    spots[0, 0:STEPS] = row_ref[...].astype(jnp.float32) + (row_bin.astype(jnp.float32) + 0.5) / BINS
    spots[0, STEPS:] = col_ref[...].astype(jnp.float32) + ((bins - row_bin * BINS).astype(jnp.float32) + 0.5) / BINS
    charges[0] = charge_ref[...]
    plane_barrier(rows, dom)

    def pair(shift):
        _, device = plane_peer(rows, dom, shift)
        return (
            pltpu.make_async_remote_copy(
                src_ref=spots.at[0], dst_ref=spots.at[shift], send_sem=send.at[shift], recv_sem=recv.at[shift],
                device_id=device, device_id_type=MESH),
            pltpu.make_async_remote_copy(
                src_ref=charge_ref, dst_ref=charges.at[shift], send_sem=send_c.at[shift],
                recv_sem=recv_c.at[shift], device_id=device, device_id_type=MESH))

    for shift in range(1, n):
        for copy in pair(shift):
            copy.start()
    total[...] = jnp.zeros_like(total)

    def add(shift):
        charge = charges[shift].astype(jnp.bfloat16)
        for s in range(STEPS):
            row = hat(r * band, band, spots[shift, s:s + 1, :]) * charge
            col = hat(d * width, width, spots[shift, STEPS + s:STEPS + s + 1, :])
            total[STEPS - 1 - s] += lax.dot_general(row, col, NT, preferred_element_type=jnp.float32)

    add(0)

    def step(shift, carry):
        for copy in pair(shift):
            copy.wait_recv()
        add(shift)
        return carry

    lax.fori_loop(1, n, step, 0)
    out[...] = total[...].astype(out.dtype)
    for shift in range(1, n):
        for copy in pair(shift):
            copy.wait_send()


def deposit(row_index, col_index, bin_index, charge, rows, dom, band, width):
    n = rows * dom
    own = row_index.shape[1]
    tile = (STEPS, band, width)
    return pl.pallas_call(
        functools.partial(gather_kernel, rows, dom),
        out_shape=(jax.ShapeDtypeStruct((n, 2 * STEPS, own), jnp.float32),
                   jax.ShapeDtypeStruct(tile, jnp.bfloat16)),
        in_specs=[VM] * 4, out_specs=(VM, VM),
        scratch_shapes=[pltpu.VMEM((n, 1, own), charge.dtype), pltpu.VMEM(tile, jnp.float32)]
        + [pltpu.SemaphoreType.DMA((n,))] * 4,
        compiler_params=pltpu.CompilerParams(collective_id=1, has_side_effects=True),
    )(row_index, col_index, bin_index, charge)


def field_kernel(hist, rows, dom, part, old_ref, cols_ref, rows_ref, parts, own_out, newest,
                 out, arrived, summed, grids, cols, rows_in, total, load,
                 sem_hs, sem_hr, sem_cs, sem_cr, sem_xs, sem_xr, sem_ps, sem_pr, sem_fs, sem_fr):
    lags, width, _ = cols.shape
    band = part.shape[1]
    piece = NG // rows
    loads = (pltpu.make_async_copy(old_ref, grids.at[pl.ds(STEPS, lags)], load.at[0]),
             pltpu.make_async_copy(cols_ref, cols, load.at[1]),
             pltpu.make_async_copy(rows_ref, rows_in, load.at[2]))
    for copy in loads:
        copy.start()
    h, r, d = place()
    chips = dom // CORES
    up, down = (h + 1, r, d), (h - 1, r, d)
    partner = (h, r, d + 1 - 2 * lax.rem(d, CORES))
    is_first, is_last = h == 0, h == hist - 1
    barrier = pltpu.get_barrier_semaphore()

    @pl.when(jnp.logical_not(is_last))
    def _():
        pl.semaphore_signal(barrier, inc=1, device_id=up, device_id_type=MESH)

    @pl.when(jnp.logical_not(is_first))
    def _():
        pl.semaphore_signal(barrier, inc=1, device_id=down, device_id_type=MESH)

    across = [(h, r, lax.rem(d + CORES * j, dom)) for j in range(1, chips)]
    pl.semaphore_signal(barrier, inc=1, device_id=partner, device_id_type=MESH)
    for device in across:
        pl.semaphore_signal(barrier, inc=1, device_id=device, device_id_type=MESH)
    count = chips + jnp.where(is_first, 0, 1) + jnp.where(is_last, 0, 1)
    pl.semaphore_wait(barrier, count)

    def remote(src, dst, s_sem, r_sem, device):
        return pltpu.make_async_remote_copy(src_ref=src, dst_ref=dst, send_sem=s_sem, recv_sem=r_sem,
                                            device_id=device, device_id_type=MESH)

    def tail_copy(c):
        columns = pl.ds(pl.multiple_of(d * width, width), width)
        return remote(old_ref.at[lags - STEPS + c, :, columns], out.at[d, c], sem_hs.at[c], sem_hr.at[c], up)

    def chain_copy(src, c):
        return remote(src.at[c], arrived.at[c], sem_cs.at[c], sem_cr.at[c], down)

    def cross_copy(c, j):
        return remote(out.at[d, c], out.at[d, c], sem_xs.at[c, j], sem_xr.at[c, j], across[j - 1])

    def partner_copy(c):
        return remote(out.at[d, c], out.at[d, c], sem_ps.at[c], sem_pr.at[c], partner)

    def forward_copy(c, j):
        other = lax.rem(d + CORES * (chips - j), dom)
        return remote(out.at[other, c], out.at[other, c], sem_fs.at[c, j], sem_fr.at[c, j], partner)

    @pl.when(is_last)
    def _():
        for c in range(STEPS):
            chain_copy(part, c).start()

    @pl.when(jnp.logical_not(is_last))
    def _():
        for c in range(STEPS):
            tail_copy(c).start()

    def products(k, first, steps):
        window = grids[pl.ds(k + STEPS - first - steps, steps)].reshape(steps * band, NG)
        mixed = lax.dot_general(cols[k], window, NT, preferred_element_type=jnp.float32).astype(part.dtype)
        stacked = jnp.concatenate(
            [mixed[:, (steps - 1 - s) * band:(steps - s) * band] for s in range(steps)], axis=0)
        span = slice(first * width, (first + steps) * width)
        for comp in range(2):
            total[comp, span] += jnp.dot(stacked, rows_in[k, comp], preferred_element_type=jnp.float32)

    def travel():
        for c in range(STEPS):
            @pl.when(jnp.logical_not(is_last))
            def _():
                chain_copy(part, c).wait_recv()
                both = part[c].astype(jnp.float32) + arrived[c].astype(jnp.float32)

                @pl.when(is_first)
                def _():
                    out[d, c] = both.astype(out.dtype)

                @pl.when(jnp.logical_not(is_first))
                def _():
                    summed[c] = both.astype(out.dtype)
                    chain_copy(summed, c).start()

            @pl.when(jnp.logical_not(is_first))
            def _():
                tail_copy(c).wait_recv()

            for j in range(1, chips):
                cross_copy(c, j).start()
            partner_copy(c).start()
        for c in range(STEPS):
            for j in range(1, chips):
                cross_copy(c, j).wait_recv()
                forward_copy(c, j).start()

    def compute():
        total[...] = jnp.zeros_like(total)
        for copy in loads:
            copy.wait()

        def lag(k, carry):
            products(k, 0, STEPS)
            return carry

        lax.fori_loop(STEPS, lags, lag, 0)
        for k in range(1, STEPS):
            products(k, 0, k)

    def phase(turn, carry):
        now = jnp.logical_xor(turn == 0, is_first)

        @pl.when(now)
        def _():
            travel()

        @pl.when(jnp.logical_not(now))
        def _():
            compute()

        return carry

    lax.fori_loop(0, 2, phase, 0)
    for c in range(STEPS):
        partner_copy(c).wait_recv()
        for j in range(1, chips):
            forward_copy(c, j).wait_recv()
    for e in range(dom):
        grids[0:STEPS, :, e * width:(e + 1) * width] = out[e]
    newest[...] = grids[0:STEPS]
    for k in range(STEPS):
        products(k, k, STEPS - k)
    for q in range(rows):
        block = jnp.concatenate([total[comp, :, q * piece:(q + 1) * piece] for comp in range(2)], axis=1)
        parts[q] = block.astype(parts.dtype)

        @pl.when(r == q)
        def _():
            own_out[...] = block

    for c in range(STEPS):
        partner_copy(c).wait_send()
        for j in range(1, chips):
            forward_copy(c, j).wait_send()
            cross_copy(c, j).wait_send()

    @pl.when(jnp.logical_not(is_first))
    def _():
        for c in range(STEPS):
            chain_copy(part, c).wait_send()

    @pl.when(jnp.logical_not(is_last))
    def _():
        for c in range(STEPS):
            tail_copy(c).wait_send()


def field_parts(part, old, kernel_cols, rows_t, hist, rows, dom):
    lags, width, _ = kernel_cols.shape
    band = old.shape[1]
    chips = dom // CORES
    dma = pltpu.SemaphoreType.DMA
    anywhere = pl.BlockSpec(memory_space=pl.ANY)
    wide = (STEPS * width, 2 * NG // rows)
    return pl.pallas_call(
        functools.partial(field_kernel, hist, rows, dom),
        out_shape=(jax.ShapeDtypeStruct((rows,) + wide, jnp.bfloat16),
                   jax.ShapeDtypeStruct(wide, jnp.float32),
                   jax.ShapeDtypeStruct((STEPS, band, NG), old.dtype)),
        in_specs=[VM, anywhere, anywhere, anywhere], out_specs=(VM, VM, VM),
        scratch_shapes=[pltpu.VMEM((dom,) + part.shape, part.dtype), pltpu.VMEM(part.shape, part.dtype),
                        pltpu.VMEM(part.shape, part.dtype),
                        pltpu.VMEM((lags + STEPS, band, NG), old.dtype),
                        pltpu.VMEM(kernel_cols.shape, kernel_cols.dtype),
                        pltpu.VMEM(rows_t.shape, rows_t.dtype),
                        pltpu.VMEM((2, STEPS * width, NG), jnp.float32), dma((3,))]
        + [dma((STEPS,))] * 4 + [dma((STEPS, chips))] * 2 + [dma((STEPS,))] * 2 + [dma((STEPS, chips))] * 2,
        compiler_params=pltpu.CompilerParams(collective_id=2, has_side_effects=True),
    )(part, old, kernel_cols, rows_t)


def sum_kernel(hist, rows, dom, parts, own, spots, momentum, out, got, mine, from_low, from_high, to_high, to_low,
               kicks, got_kicks, sem_ys, sem_yr, sem_us, sem_ur, sem_ds, sem_dr, sem_ks, sem_kr):
    h, r, d = place()
    n = rows * dom
    tall, wide = own.shape
    width, band = tall // STEPS, wide // 2
    size = tall // PIECES
    kind = parts.dtype
    up, down = (h + 1, r, d), (h - 1, r, d)
    is_first, is_last = h == 0, h == hist - 1
    inner = jnp.logical_and(h > 0, h < hist - 1)
    barrier = pltpu.get_barrier_semaphore()

    @pl.when(jnp.logical_not(is_last))
    def _():
        pl.semaphore_signal(barrier, inc=1, device_id=up, device_id_type=MESH)

    @pl.when(jnp.logical_not(is_first))
    def _():
        pl.semaphore_signal(barrier, inc=1, device_id=down, device_id_type=MESH)

    for shift in range(1, n):
        pl.semaphore_signal(barrier, inc=1, device_id=plane_peer(rows, dom, shift)[1], device_id_type=MESH)
    pl.semaphore_wait(barrier, n - 1 + jnp.where(is_first, 0, 1) + jnp.where(is_last, 0, 1))

    def span(c):
        return pl.ds(pl.multiple_of(c * size, size), size)

    def row_copy(c, j):
        other = lax.rem(r + j, rows)
        return pltpu.make_async_remote_copy(
            src_ref=parts.at[other, span(c)], dst_ref=got.at[j, span(c)], send_sem=sem_ys.at[c, j],
            recv_sem=sem_yr.at[c, j], device_id=(h, other, d), device_id_type=MESH)

    def up_copy(c):
        return pltpu.make_async_remote_copy(
            src_ref=to_high.at[span(c)], dst_ref=from_low.at[span(c)], send_sem=sem_us.at[c],
            recv_sem=sem_ur.at[c], device_id=up, device_id_type=MESH)

    def down_copy(c):
        return pltpu.make_async_remote_copy(
            src_ref=to_low.at[span(c)], dst_ref=from_high.at[span(c)], send_sem=sem_ds.at[c],
            recv_sem=sem_dr.at[c], device_id=down, device_id_type=MESH)

    for c in range(PIECES):
        for j in range(1, rows):
            row_copy(c, j).start()

    kicks[...] = jnp.zeros_like(kicks)

    def kick(s):
        rows_s = pl.ds(pl.multiple_of(s * width, width), width)
        value = mine[rows_s]
        stacked = jnp.concatenate([value[:, :band], value[:, band:]], axis=0)
        coarse = stacked.astype(kind)
        fine = (stacked - coarse.astype(jnp.float32)).astype(kind)
        table = jnp.concatenate([coarse, fine], axis=0)

        def block(k, carry):
            row = hat(r * band, band, spots[k, pl.ds(s, 1), :])
            col = hat(d * width, width, spots[k, pl.ds(STEPS + s, 1), :]).astype(jnp.float32)
            along = jnp.dot(table, row, preferred_element_type=jnp.float32)
            for comp in range(2):
                both = (along[comp * width:(comp + 1) * width]
                        + along[(2 + comp) * width:(3 + comp) * width])
                kicks[k, comp:comp + 1, :] += jnp.sum(both * col, axis=0, keepdims=True)
            return carry

        lax.fori_loop(0, n, block, 0)

    lag = 2 * (hist - 2)
    group = PIECES // STEPS

    def step(t, carry):
        @pl.when(t < PIECES)
        def _():
            value = own[span(t)]
            for j in range(1, rows):
                row_copy(t, j).wait_recv()
                value += got[j, span(t)].astype(jnp.float32)
            mine[span(t)] = value

            @pl.when(is_first)
            def _():
                to_high[span(t)] = value.astype(kind)
                up_copy(t).start()

            @pl.when(is_last)
            def _():
                to_low[span(t)] = value.astype(kind)
                down_copy(t).start()

        low = t - 2 * h

        @pl.when(jnp.logical_and(inner, jnp.logical_and(low >= 0, low < PIECES)))
        def _():
            up_copy(low).wait_recv()
            to_high[span(low)] = (mine[span(low)] + from_low[span(low)].astype(jnp.float32)).astype(kind)
            up_copy(low).start()

        high = t - 2 * (hist - 1 - h)

        @pl.when(jnp.logical_and(inner, jnp.logical_and(high >= 0, high < PIECES)))
        def _():
            down_copy(high).wait_recv()
            to_low[span(high)] = (mine[span(high)] + from_high[span(high)].astype(jnp.float32)).astype(kind)
            down_copy(high).start()

        done = t - lag

        @pl.when(done >= 0)
        def _():
            @pl.when(is_first)
            def _():
                down_copy(done).wait_recv()
                mine[span(done)] = mine[span(done)] + from_high[span(done)].astype(jnp.float32)

            @pl.when(is_last)
            def _():
                up_copy(done).wait_recv()
                mine[span(done)] = mine[span(done)] + from_low[span(done)].astype(jnp.float32)

            @pl.when(inner)
            def _():
                mine[span(done)] = (mine[span(done)] + from_low[span(done)].astype(jnp.float32)
                                    + from_high[span(done)].astype(jnp.float32))

            @pl.when(lax.rem(done, group) == group - 1)
            def _():
                kick(done // group)

        return carry

    lax.fori_loop(0, PIECES + lag, step, 0)

    def kick_copy(k):
        _, device = plane_peer(rows, dom, n - k)
        return pltpu.make_async_remote_copy(
            src_ref=kicks.at[k], dst_ref=got_kicks.at[k], send_sem=sem_ks.at[k], recv_sem=sem_kr.at[k],
            device_id=device, device_id_type=MESH)

    for k in range(1, n):
        kick_copy(k).start()

    def finish(c, carry):
        @pl.when(jnp.logical_not(is_last))
        def _():
            up_copy(c).wait_send()

        @pl.when(jnp.logical_not(is_first))
        def _():
            down_copy(c).wait_send()

        for j in range(1, rows):
            row_copy(c, j).wait_send()
        return carry

    lax.fori_loop(0, PIECES, finish, 0)
    total = kicks[0]
    for k in range(1, n):
        kick_copy(k).wait()
        total = total + got_kicks[k]
    out[...] = momentum[...] + kick_scale * total


def sum_and_kick(parts, own, spots, momentum, hist, rows, dom):
    tall, wide = own.shape
    n = rows * dom
    dma = pltpu.SemaphoreType.DMA
    flat = pltpu.VMEM((tall, wide), parts.dtype)
    each = pltpu.VMEM((n,) + momentum.shape, momentum.dtype)
    return pl.pallas_call(
        functools.partial(sum_kernel, hist, rows, dom),
        out_shape=jax.ShapeDtypeStruct(momentum.shape, momentum.dtype),
        in_specs=[VM] * 4, out_specs=VM,
        scratch_shapes=[pltpu.VMEM(parts.shape, parts.dtype), pltpu.VMEM((tall, wide), jnp.float32),
                        flat, flat, flat, flat, each, each]
        + [dma((PIECES, rows))] * 2 + [dma((PIECES,))] * 4 + [dma((n,))] * 2,
        compiler_params=pltpu.CompilerParams(collective_id=3, has_side_effects=True),
    )(parts, own, spots, momentum)


def local(hist, rows, dom, row_index, col_index, bin_index, charge, momentum, history, kernel_cols, kernel_rows):
    band = history.shape[1]
    width = kernel_cols.shape[1]
    spots, part = deposit(row_index, col_index, bin_index, charge.astype(jnp.float32)[None], rows, dom, band, width)
    rows_t = jnp.transpose(kernel_rows, (0, 2, 1, 3))
    parts, own, newest = field_parts(part, history, kernel_cols, rows_t, hist, rows, dom)
    cycle_now = jnp.concatenate([newest, history[:-STEPS]], axis=0)
    return sum_and_kick(parts, own, spots, momentum, hist, rows, dom), cycle_now


def solution(mesh):
    spread = ("hist", "rows", "dom")
    in_specs = (P(None, spread), P(None, spread), P(None, spread), P(spread), P(None, spread),
                P("hist", "rows", None), P("hist", "dom", None), P("hist", "rows", None, None))
    out_specs = (P(None, spread), P("hist", "rows", None))
    sizes = mesh.shape
    body = functools.partial(local, sizes["hist"], sizes["rows"], sizes["dom"])
    return jax.shard_map(body, mesh=mesh, in_specs=in_specs, out_specs=out_specs, check_vma=False)
```

```python
import functools
import jax
import jax.numpy as jnp
from jax import lax
from jax.experimental import pallas as pl
from jax.experimental.pallas import tpu as pltpu
from jax.sharding import PartitionSpec as P

NG = 512
BINS = 16
STEPS = 4
CORES = 2
PIECES = 8
kick_scale = 0.5

MESH = pl.DeviceIdType.MESH
VM = pl.BlockSpec(memory_space=pltpu.VMEM)
NT = (((1,), (1,)), ((), ()))


def place():
    return lax.axis_index("hist"), lax.axis_index("rows"), lax.axis_index("dom")


def hat(first, extent, where):
    places = lax.broadcasted_iota(jnp.int32, (extent, where.shape[1]), 0) + first
    gap = (places.astype(jnp.float32) - where).astype(jnp.bfloat16)
    return jnp.maximum(jnp.bfloat16(1.0) - jnp.abs(gap), jnp.bfloat16(0.0))


def plane_peer(rows, dom, shift):
    h, r, d = place()
    other = lax.rem(r * dom + d + shift, rows * dom)
    return other, (h, other // dom, lax.rem(other, dom))


def plane_barrier(rows, dom):
    barrier = pltpu.get_barrier_semaphore()
    for shift in range(1, rows * dom):
        pl.semaphore_signal(barrier, inc=1, device_id=plane_peer(rows, dom, shift)[1], device_id_type=MESH)
    pl.semaphore_wait(barrier, rows * dom - 1)


def gather_kernel(rows, dom, row_ref, col_ref, bin_ref, charge_ref, spots, out, charges, total,
                  send, recv, send_c, recv_c):
    _, r, d = place()
    n = rows * dom
    _, band, width = out.shape
    bins = bin_ref[...]
    row_bin = bins // BINS
    spots[0, 0:STEPS] = row_ref[...].astype(jnp.float32) + (row_bin.astype(jnp.float32) + 0.5) / BINS
    spots[0, STEPS:] = col_ref[...].astype(jnp.float32) + ((bins - row_bin * BINS).astype(jnp.float32) + 0.5) / BINS
    charges[0] = charge_ref[...]
    plane_barrier(rows, dom)

    def pair(shift):
        _, device = plane_peer(rows, dom, shift)
        return (
            pltpu.make_async_remote_copy(
                src_ref=spots.at[0], dst_ref=spots.at[shift], send_sem=send.at[shift], recv_sem=recv.at[shift],
                device_id=device, device_id_type=MESH),
            pltpu.make_async_remote_copy(
                src_ref=charge_ref, dst_ref=charges.at[shift], send_sem=send_c.at[shift],
                recv_sem=recv_c.at[shift], device_id=device, device_id_type=MESH))

    for shift in range(1, n):
        for copy in pair(shift):
            copy.start()
    total[...] = jnp.zeros_like(total)

    def add(shift):
        charge = charges[shift].astype(jnp.bfloat16)
        for s in range(STEPS):
            row = hat(r * band, band, spots[shift, s:s + 1, :]) * charge
            col = hat(d * width, width, spots[shift, STEPS + s:STEPS + s + 1, :])
            total[STEPS - 1 - s] += lax.dot_general(row, col, NT, preferred_element_type=jnp.float32)

    add(0)

    def step(shift, carry):
        for copy in pair(shift):
            copy.wait_recv()
        add(shift)
        return carry

    lax.fori_loop(1, n, step, 0)
    out[...] = total[...].astype(out.dtype)
    for shift in range(1, n):
        for copy in pair(shift):
            copy.wait_send()


def deposit(row_index, col_index, bin_index, charge, rows, dom, band, width):
    n = rows * dom
    own = row_index.shape[1]
    tile = (STEPS, band, width)
    return pl.pallas_call(
        functools.partial(gather_kernel, rows, dom),
        out_shape=(jax.ShapeDtypeStruct((n, 2 * STEPS, own), jnp.float32),
                   jax.ShapeDtypeStruct(tile, jnp.bfloat16)),
        in_specs=[VM] * 4, out_specs=(VM, VM),
        scratch_shapes=[pltpu.VMEM((n, 1, own), charge.dtype), pltpu.VMEM(tile, jnp.float32)]
        + [pltpu.SemaphoreType.DMA((n,))] * 4,
        compiler_params=pltpu.CompilerParams(collective_id=1, has_side_effects=True),
    )(row_index, col_index, bin_index, charge)


def field_kernel(hist, rows, dom, part, old_ref, cols_ref, rows_ref, parts, own_out, newest,
                 out, arrived, summed, grids, cols, rows_in, total, load,
                 sem_hs, sem_hr, sem_cs, sem_cr, sem_xs, sem_xr, sem_ps, sem_pr, sem_fs, sem_fr):
    lags, width, _ = cols.shape
    band = part.shape[1]
    piece = NG // rows
    loads = (pltpu.make_async_copy(old_ref, grids.at[pl.ds(STEPS, lags)], load.at[0]),
             pltpu.make_async_copy(cols_ref, cols, load.at[1]),
             pltpu.make_async_copy(rows_ref, rows_in, load.at[2]))
    for copy in loads:
        copy.start()
    h, r, d = place()
    chips = dom // CORES
    up, down = (h + 1, r, d), (h - 1, r, d)
    partner = (h, r, d + 1 - 2 * lax.rem(d, CORES))
    is_first, is_last = h == 0, h == hist - 1
    barrier = pltpu.get_barrier_semaphore()

    @pl.when(jnp.logical_not(is_last))
    def _():
        pl.semaphore_signal(barrier, inc=1, device_id=up, device_id_type=MESH)

    @pl.when(jnp.logical_not(is_first))
    def _():
        pl.semaphore_signal(barrier, inc=1, device_id=down, device_id_type=MESH)

    across = [(h, r, lax.rem(d + CORES * j, dom)) for j in range(1, chips)]
    pl.semaphore_signal(barrier, inc=1, device_id=partner, device_id_type=MESH)
    for device in across:
        pl.semaphore_signal(barrier, inc=1, device_id=device, device_id_type=MESH)
    count = chips + jnp.where(is_first, 0, 1) + jnp.where(is_last, 0, 1)
    pl.semaphore_wait(barrier, count)

    def remote(src, dst, s_sem, r_sem, device):
        return pltpu.make_async_remote_copy(src_ref=src, dst_ref=dst, send_sem=s_sem, recv_sem=r_sem,
                                            device_id=device, device_id_type=MESH)

    def tail_copy(c):
        columns = pl.ds(pl.multiple_of(d * width, width), width)
        return remote(old_ref.at[lags - STEPS + c, :, columns], out.at[d, c], sem_hs.at[c], sem_hr.at[c], up)

    def chain_copy(src, c):
        return remote(src.at[c], arrived.at[c], sem_cs.at[c], sem_cr.at[c], down)

    def cross_copy(c, j):
        return remote(out.at[d, c], out.at[d, c], sem_xs.at[c, j], sem_xr.at[c, j], across[j - 1])

    def partner_copy(c):
        return remote(out.at[d, c], out.at[d, c], sem_ps.at[c], sem_pr.at[c], partner)

    def forward_copy(c, j):
        other = lax.rem(d + CORES * (chips - j), dom)
        return remote(out.at[other, c], out.at[other, c], sem_fs.at[c, j], sem_fr.at[c, j], partner)

    @pl.when(is_last)
    def _():
        for c in range(STEPS):
            chain_copy(part, c).start()

    @pl.when(jnp.logical_not(is_last))
    def _():
        for c in range(STEPS):
            tail_copy(c).start()

    def products(k, first, steps):
        window = grids[pl.ds(k + STEPS - first - steps, steps)].reshape(steps * band, NG)
        mixed = lax.dot_general(cols[k], window, NT, preferred_element_type=jnp.float32).astype(part.dtype)
        stacked = jnp.concatenate(
            [mixed[:, (steps - 1 - s) * band:(steps - s) * band] for s in range(steps)], axis=0)
        span = slice(first * width, (first + steps) * width)
        for comp in range(2):
            total[comp, span] += jnp.dot(stacked, rows_in[k, comp], preferred_element_type=jnp.float32)

    def travel():
        for c in range(STEPS):
            @pl.when(jnp.logical_not(is_last))
            def _():
                chain_copy(part, c).wait_recv()
                both = part[c].astype(jnp.float32) + arrived[c].astype(jnp.float32)

                @pl.when(is_first)
                def _():
                    out[d, c] = both.astype(out.dtype)

                @pl.when(jnp.logical_not(is_first))
                def _():
                    summed[c] = both.astype(out.dtype)
                    chain_copy(summed, c).start()

            @pl.when(jnp.logical_not(is_first))
            def _():
                tail_copy(c).wait_recv()

            for j in range(1, chips):
                cross_copy(c, j).start()
            partner_copy(c).start()
        for c in range(STEPS):
            for j in range(1, chips):
                cross_copy(c, j).wait_recv()
                forward_copy(c, j).start()

    def compute():
        total[...] = jnp.zeros_like(total)
        for copy in loads:
            copy.wait()

        def lag(k, carry):
            products(k, 0, STEPS)
            return carry

        lax.fori_loop(STEPS, lags, lag, 0)
        for k in range(1, STEPS):
            products(k, 0, k)

    def phase(turn, carry):
        now = jnp.logical_xor(turn == 0, is_first)

        @pl.when(now)
        def _():
            travel()

        @pl.when(jnp.logical_not(now))
        def _():
            compute()

        return carry

    lax.fori_loop(0, 2, phase, 0)
    for c in range(STEPS):
        partner_copy(c).wait_recv()
        for j in range(1, chips):
            forward_copy(c, j).wait_recv()
    for e in range(dom):
        grids[0:STEPS, :, e * width:(e + 1) * width] = out[e]
    newest[...] = grids[0:STEPS]
    for k in range(STEPS):
        products(k, k, STEPS - k)
    for q in range(rows):
        block = jnp.concatenate([total[comp, :, q * piece:(q + 1) * piece] for comp in range(2)], axis=1)
        parts[q] = block.astype(parts.dtype)

        @pl.when(r == q)
        def _():
            own_out[...] = block

    for c in range(STEPS):
        partner_copy(c).wait_send()
        for j in range(1, chips):
            forward_copy(c, j).wait_send()
            cross_copy(c, j).wait_send()

    @pl.when(jnp.logical_not(is_first))
    def _():
        for c in range(STEPS):
            chain_copy(part, c).wait_send()

    @pl.when(jnp.logical_not(is_last))
    def _():
        for c in range(STEPS):
            tail_copy(c).wait_send()


def field_parts(part, old, kernel_cols, rows_t, hist, rows, dom):
    lags, width, _ = kernel_cols.shape
    band = old.shape[1]
    chips = dom // CORES
    dma = pltpu.SemaphoreType.DMA
    anywhere = pl.BlockSpec(memory_space=pl.ANY)
    wide = (STEPS * width, 2 * NG // rows)
    return pl.pallas_call(
        functools.partial(field_kernel, hist, rows, dom),
        out_shape=(jax.ShapeDtypeStruct((rows,) + wide, jnp.bfloat16),
                   jax.ShapeDtypeStruct(wide, jnp.float32),
                   jax.ShapeDtypeStruct((STEPS, band, NG), old.dtype)),
        in_specs=[VM, anywhere, anywhere, anywhere], out_specs=(VM, VM, VM),
        scratch_shapes=[pltpu.VMEM((dom,) + part.shape, part.dtype), pltpu.VMEM(part.shape, part.dtype),
                        pltpu.VMEM(part.shape, part.dtype),
                        pltpu.VMEM((lags + STEPS, band, NG), old.dtype),
                        pltpu.VMEM(kernel_cols.shape, kernel_cols.dtype),
                        pltpu.VMEM(rows_t.shape, rows_t.dtype),
                        pltpu.VMEM((2, STEPS * width, NG), jnp.float32), dma((3,))]
        + [dma((STEPS,))] * 4 + [dma((STEPS, chips))] * 2 + [dma((STEPS,))] * 2 + [dma((STEPS, chips))] * 2,
        compiler_params=pltpu.CompilerParams(collective_id=2, has_side_effects=True),
    )(part, old, kernel_cols, rows_t)


def sum_kernel(hist, rows, dom, parts, own, spots, momentum, out, got, mine, from_low, from_high, to_high, to_low,
               kicks, got_kicks, sem_ys, sem_yr, sem_us, sem_ur, sem_ds, sem_dr, sem_ks, sem_kr):
    h, r, d = place()
    n = rows * dom
    tall, wide = own.shape
    width, band = tall // STEPS, wide // 2
    size = tall // PIECES
    kind = parts.dtype
    up, down = (h + 1, r, d), (h - 1, r, d)
    is_first, is_last = h == 0, h == hist - 1
    inner = jnp.logical_and(h > 0, h < hist - 1)
    barrier = pltpu.get_barrier_semaphore()

    @pl.when(jnp.logical_not(is_last))
    def _():
        pl.semaphore_signal(barrier, inc=1, device_id=up, device_id_type=MESH)

    @pl.when(jnp.logical_not(is_first))
    def _():
        pl.semaphore_signal(barrier, inc=1, device_id=down, device_id_type=MESH)

    for shift in range(1, n):
        pl.semaphore_signal(barrier, inc=1, device_id=plane_peer(rows, dom, shift)[1], device_id_type=MESH)
    pl.semaphore_wait(barrier, n - 1 + jnp.where(is_first, 0, 1) + jnp.where(is_last, 0, 1))

    def span(c):
        return pl.ds(pl.multiple_of(c * size, size), size)

    def row_copy(c, j):
        other = lax.rem(r + j, rows)
        return pltpu.make_async_remote_copy(
            src_ref=parts.at[other, span(c)], dst_ref=got.at[j, span(c)], send_sem=sem_ys.at[c, j],
            recv_sem=sem_yr.at[c, j], device_id=(h, other, d), device_id_type=MESH)

    def up_copy(c):
        return pltpu.make_async_remote_copy(
            src_ref=to_high.at[span(c)], dst_ref=from_low.at[span(c)], send_sem=sem_us.at[c],
            recv_sem=sem_ur.at[c], device_id=up, device_id_type=MESH)

    def down_copy(c):
        return pltpu.make_async_remote_copy(
            src_ref=to_low.at[span(c)], dst_ref=from_high.at[span(c)], send_sem=sem_ds.at[c],
            recv_sem=sem_dr.at[c], device_id=down, device_id_type=MESH)

    for c in range(PIECES):
        for j in range(1, rows):
            row_copy(c, j).start()

    kicks[...] = jnp.zeros_like(kicks)

    def kick(s):
        rows_s = pl.ds(pl.multiple_of(s * width, width), width)
        value = mine[rows_s]
        stacked = jnp.concatenate([value[:, :band], value[:, band:]], axis=0)
        coarse = stacked.astype(kind)
        fine = (stacked - coarse.astype(jnp.float32)).astype(kind)
        table = jnp.concatenate([coarse, fine], axis=0)

        def block(k, carry):
            row = hat(r * band, band, spots[k, pl.ds(s, 1), :])
            col = hat(d * width, width, spots[k, pl.ds(STEPS + s, 1), :]).astype(jnp.float32)
            along = jnp.dot(table, row, preferred_element_type=jnp.float32)
            for comp in range(2):
                both = (along[comp * width:(comp + 1) * width]
                        + along[(2 + comp) * width:(3 + comp) * width])
                kicks[k, comp:comp + 1, :] += jnp.sum(both * col, axis=0, keepdims=True)
            return carry

        lax.fori_loop(0, n, block, 0, unroll=8)

    lag = 2 * (hist - 2)
    group = PIECES // STEPS
    late = lag + 3

    def step(t, carry):
        @pl.when(t < PIECES)
        def _():
            value = own[span(t)]
            for j in range(1, rows):
                row_copy(t, j).wait_recv()
                value += got[j, span(t)].astype(jnp.float32)
            mine[span(t)] = value

            @pl.when(is_first)
            def _():
                to_high[span(t)] = value.astype(kind)
                up_copy(t).start()

            @pl.when(is_last)
            def _():
                to_low[span(t)] = value.astype(kind)
                down_copy(t).start()

        low = t - 2 * h

        @pl.when(jnp.logical_and(inner, jnp.logical_and(low >= 0, low < PIECES)))
        def _():
            up_copy(low).wait_recv()
            to_high[span(low)] = (mine[span(low)] + from_low[span(low)].astype(jnp.float32)).astype(kind)
            up_copy(low).start()

        high = t - 2 * (hist - 1 - h)

        @pl.when(jnp.logical_and(inner, jnp.logical_and(high >= 0, high < PIECES)))
        def _():
            down_copy(high).wait_recv()
            to_low[span(high)] = (mine[span(high)] + from_high[span(high)].astype(jnp.float32)).astype(kind)
            down_copy(high).start()

        done = t - late

        @pl.when(done >= 0)
        def _():
            @pl.when(is_first)
            def _():
                down_copy(done).wait_recv()
                mine[span(done)] = mine[span(done)] + from_high[span(done)].astype(jnp.float32)

            @pl.when(is_last)
            def _():
                up_copy(done).wait_recv()
                mine[span(done)] = mine[span(done)] + from_low[span(done)].astype(jnp.float32)

            @pl.when(inner)
            def _():
                mine[span(done)] = (mine[span(done)] + from_low[span(done)].astype(jnp.float32)
                                    + from_high[span(done)].astype(jnp.float32))

            @pl.when(lax.rem(done, group) == group - 1)
            def _():
                kick(done // group)

        return carry

    lax.fori_loop(0, PIECES + late, step, 0)

    def kick_copy(k):
        _, device = plane_peer(rows, dom, n - k)
        return pltpu.make_async_remote_copy(
            src_ref=kicks.at[k], dst_ref=got_kicks.at[k], send_sem=sem_ks.at[k], recv_sem=sem_kr.at[k],
            device_id=device, device_id_type=MESH)

    for k in range(1, n):
        kick_copy(k).start()

    def finish(c, carry):
        @pl.when(jnp.logical_not(is_last))
        def _():
            up_copy(c).wait_send()

        @pl.when(jnp.logical_not(is_first))
        def _():
            down_copy(c).wait_send()

        for j in range(1, rows):
            row_copy(c, j).wait_send()
        return carry

    lax.fori_loop(0, PIECES, finish, 0)
    total = kicks[0]
    for k in range(1, n):
        kick_copy(k).wait()
        total = total + got_kicks[k]
    out[...] = momentum[...] + kick_scale * total


def sum_and_kick(parts, own, spots, momentum, hist, rows, dom):
    tall, wide = own.shape
    n = rows * dom
    dma = pltpu.SemaphoreType.DMA
    flat = pltpu.VMEM((tall, wide), parts.dtype)
    each = pltpu.VMEM((n,) + momentum.shape, momentum.dtype)
    return pl.pallas_call(
        functools.partial(sum_kernel, hist, rows, dom),
        out_shape=jax.ShapeDtypeStruct(momentum.shape, momentum.dtype),
        in_specs=[VM] * 4, out_specs=VM,
        scratch_shapes=[pltpu.VMEM(parts.shape, parts.dtype), pltpu.VMEM((tall, wide), jnp.float32),
                        flat, flat, flat, flat, each, each]
        + [dma((PIECES, rows))] * 2 + [dma((PIECES,))] * 4 + [dma((n,))] * 2,
        compiler_params=pltpu.CompilerParams(collective_id=3, has_side_effects=True),
    )(parts, own, spots, momentum)


def local(hist, rows, dom, row_index, col_index, bin_index, charge, momentum, history, kernel_cols, kernel_rows):
    band = history.shape[1]
    width = kernel_cols.shape[1]
    spots, part = deposit(row_index, col_index, bin_index, charge.astype(jnp.float32)[None], rows, dom, band, width)
    rows_t = jnp.transpose(kernel_rows, (0, 2, 1, 3))
    parts, own, newest = field_parts(part, history, kernel_cols, rows_t, hist, rows, dom)
    cycle_now = jnp.concatenate([newest, history[:-STEPS]], axis=0)
    return sum_and_kick(parts, own, spots, momentum, hist, rows, dom), cycle_now


def solution(mesh):
    spread = ("hist", "rows", "dom")
    in_specs = (P(None, spread), P(None, spread), P(None, spread), P(spread), P(None, spread),
                P("hist", "rows", None), P("hist", "dom", None), P("hist", "rows", None, None))
    out_specs = (P(None, spread), P("hist", "rows", None))
    sizes = mesh.shape
    body = functools.partial(local, sizes["hist"], sizes["rows"], sizes["dom"])
    return jax.shard_map(body, mesh=mesh, in_specs=in_specs, out_specs=out_specs, check_vma=False)
```
